32 devices in a mesh: expert: 4 (over z), shard: 8 (over y, x, core).
Axes of the slice: x: 2, y: 2, z: 4, core: 2. Of those that a mesh axis runs over, the one named last changes fastest.
Arguments:
- master_down: float32 [16, 6400, 4096], P('expert', None, 'shard'), may hold values from -0.109375 to 0.109375
- second_down: bfloat16 [16, 6400, 4096], P('expert', None, 'shard'), may hold values from -0.0390625 to 0.0390625
- router_weight: float32 [4096, 16], P('shard', 'expert'), may hold values from -0.09375 to 0.09375
- router_gain: float32 [4096], P('shard'), may hold values from 0.25 to 1.75
Outputs:
- final_down: bfloat16 [16, 6400, 4096], P('expert', 'shard')
- scale_down: float32 [16, 6400], P('expert', 'shard')
- serve_router: bfloat16 [4096, 16], replicated
The draws below stay inside these ranges and needn't reach their ends.
All inputs are finite; a program needn't handle non-finite values.
Results may differ from the reference program's by a relative error of at most 0.001.
Values may be sent and summed in bfloat16 or wider, within the bound.
No kernel may reach another device: no remote copies, remote signals or barrier semaphores. Data moves between devices by JAX's collectives and lax.ppermute only.
A program may use at most 256 MiB of HBM per device.

```python
import jax
import jax.numpy as jnp
from jax import lax

EXPERTS = 16
D_MODEL = 4096
D_EXPERT = 6400


def spiked(values, stream_key, source, target, blocks, factor):
    def block_of(position):
        return (jnp.arange(values.shape[position]) // (values.shape[position] // blocks)).reshape((-1,) + (1,) * (values.ndim - 1 - position))

    one_side = jax.random.permutation(stream_key, blocks)[block_of(target)]
    other_side = (block_of(target) + blocks // 2) % blocks
    return jnp.where((block_of(source) == one_side) | (block_of(source) == other_side), factor * values, values)


def level_of(key, shape, split, low, top_value):
    loudness, own = 1.0, jax.random.fold_in(key, 6)
    for position, parts in split:
        draws = jnp.exp(jax.random.uniform(jax.random.fold_in(own, position), (parts,), jnp.float32, low / len(split), top_value / len(split)))
        loudness = loudness * jnp.repeat(draws, shape[position] // parts).reshape([-1 if axis == position else 1 for axis in range(len(shape))])
    return loudness


def bell_draw(key, shape, width, most, shards=(), kind=jnp.bfloat16):
    entries = width * jax.random.normal(key, shape, jnp.float32)
    if shards:
        entries = entries * level_of(key, shape, shards, -0.22, 0.18)
    return jnp.clip(entries, -most, most).astype(kind)


def bell_draw_with(rng, shape, scale, most, split, heavy, dtype=jnp.bfloat16):
    array = scale * jax.random.normal(rng, shape, jnp.float32)
    if split:
        array = array * level_of(rng, shape, split, -0.22, 0.18)
    return jnp.clip(spiked(array, jax.random.fold_in(rng, 3), *heavy), -most, most).astype(dtype)


def setup_inputs(seed: int = 0) -> dict:
    splits = jax.random.split(jax.random.key(seed), 5)
    return {
        "master_down": bell_draw_with(splits[0], (EXPERTS, D_EXPERT, D_MODEL), D_EXPERT ** -0.5, 0.109375, ((0, 4), (2, 8)), (2, 1, 8, 2.0), jnp.float32),
        "second_down": bell_draw(splits[1], (EXPERTS, D_EXPERT, D_MODEL), (D_EXPERT * 4) ** -0.5, 0.0390625, ((0, 4), (2, 8))),
        "router_weight": bell_draw(splits[2], (D_MODEL, EXPERTS), D_MODEL ** -0.5, 0.09375, ((0, 8), (1, 4)), jnp.float32),
        "router_gain": jnp.clip(1.0 + 0.15 * jax.random.normal(splits[3], (D_MODEL,), jnp.float32), 0.25, 1.75),
    }


def reference(master_down, second_down, router_weight, router_gain):
    merged_down = master_down + second_down.astype(jnp.float32)
    scale_down = jnp.sqrt(lax.optimization_barrier(jnp.sum(merged_down * merged_down, axis=2)))
    final_down = (merged_down / jnp.expand_dims(scale_down, 2)).astype(jnp.bfloat16)
    serve_router = (router_weight * router_gain[:, None]).astype(jnp.bfloat16)
    return (final_down, scale_down, serve_router)
```

```python
import jax
import jax.numpy as jnp
from jax import lax
from jax.experimental import pallas as pl
from jax.experimental.pallas import tpu as pltpu
from jax.sharding import PartitionSpec as P


def row_block(rows):
    return max(d for d in range(1, 101) if rows % d == 0 and (d % 16 == 0 or d == rows or d == 1))


def place(me, parts, whole, e, low, block, shape):
    n = len(parts)
    rows, width = parts[0].shape
    first = whole is None

    def body(me_ref, *refs):
        out_ref = refs[-1]
        for k in range(n):
            column = pl.multiple_of((me_ref[0] ^ k) * width, width)
            out_ref[0, :, pl.ds(column, width)] = refs[k][...]

    return pl.pallas_call(
        body,
        out_shape=jax.ShapeDtypeStruct(shape, parts[0].dtype),
        grid_spec=pltpu.PrefetchScalarGridSpec(
            num_scalar_prefetch=1,
            grid=(rows // block,),
            in_specs=[pl.BlockSpec((block, width), lambda r, _: (r, 0))] * n
            + ([] if first else [pl.BlockSpec(memory_space=pl.ANY)]),
            out_specs=pl.BlockSpec((1, block, n * width), lambda r, _: (e, low // block + r, 0)),
        ),
        input_output_aliases={} if first else {1 + n: 0},
    )(me, *parts, *([] if first else [whole]))


def send_order(n):
    return [k for k in sorted(range(1, n), key=lambda k: (k & 1, k)) if k != 1] + [1]


def after(values, earlier):
    return lax.optimization_barrier((values, earlier))[0]


def local(master_down, second_down, router_weight, router_gain):
    experts, rows, width = master_down.shape
    n = lax.axis_size("shard")
    me = lax.axis_index("shard")
    own_rows = rows // n
    block = row_block(own_rows)
    order = send_order(n)
    early, late = order[: n // 2], order[n // 2 :]

    def swap(x, k, axis="shard"):
        return lax.ppermute(x, axis, [(i, i ^ k) for i in range(lax.axis_size(axis))])

    def squares(pair, low, high):
        m = pair[0][low:high] + pair[1][low:high].astype(jnp.float32)
        return jnp.sum(m * m, axis=2)

    def narrow(pair, scale, e, k, low, high):
        start = (me ^ k) * own_rows + low
        cut = lambda x: lax.dynamic_slice(x, (e, start, 0), (1, high - low, width))[0]
        m = cut(pair[0]) + cut(pair[1]).astype(jnp.float32)
        return (m / lax.dynamic_slice_in_dim(scale, start, high - low)[:, None]).astype(jnp.bfloat16)

    pair = (master_down, second_down)
    sums = squares(pair, 0, 1)
    scale = jnp.sqrt(jnp.sum(lax.all_gather(sums, "shard", axis=0), axis=0))[0]
    parts = [None] * n
    pair, scale0 = after((pair, scale), scale)
    for k in early:
        piece = narrow(pair, scale0, 0, k, 0, own_rows)
        parts[k] = swap(piece, k)
        pair, scale0 = after((pair, scale0), piece)

    sums = squares(pair, 1, experts)
    router = (router_weight * router_gain[:, None]).T
    cols, dim = router.shape
    mixed = jnp.concatenate([sums.reshape(-1), router.reshape(-1)])
    pair, scale0 = after((pair, scale0), mixed)
    mixes = [mixed] + [swap(mixed, k) for k in range(1, n)]
    for k in late:
        piece = narrow(pair, scale0, 0, k, 0, own_rows)
        parts[k] = swap(piece, k)
        pair, scale0 = after((pair, scale0), piece)
    parts[0] = narrow(pair, scale0, 0, 0, 0, own_rows)
    rest = mixes[0][: sums.size]
    for mix in mixes[1:]:
        rest = rest + mix[: sums.size]
    rest = jnp.sqrt(rest).reshape(sums.shape)
    wide = jnp.zeros((cols, dim * n), jnp.bfloat16)
    for k, mix in enumerate(mixes):
        got = mix[sums.size :].reshape(cols, dim).astype(jnp.bfloat16)
        wide = lax.dynamic_update_slice(wide, got, (0, (me ^ k) * dim))
    scales = [scale] + [rest[e] for e in range(experts - 1)]

    shape = (experts, own_rows, n * width)
    where = jnp.reshape(me, (1,)).astype(jnp.int32)
    chunks = [(e, 0, own_rows) for e in range(1, experts - 1)]
    chunks += [(experts - 1, 0, own_rows - 2 * block), (experts - 1, own_rows - 2 * block, own_rows)]
    arrived = [(parts, 0, 0)]
    for e, low, high in chunks:
        pair, scale = after((pair, scales[e]), scales[e])
        parts, pieces = [None] * n, []
        for group in ([order[:2], order[2:4], order[4:] + [0]] if e == 1 else [order + [0]]):
            for k in group:
                pieces.append(narrow(pair, scale, e, k, low, high))
                parts[k] = swap(pieces[-1], k) if k else pieces[-1]
            pair = after(pair, pieces)
        arrived.append((parts, e, low))
    wide = after(wide, pieces)
    whole = None
    for parts, e, low in arrived:
        whole = place(where, parts, whole, e, low, block, shape)

    m = lax.axis_size("expert")
    mine = lax.axis_index("expert")
    tall = jnp.zeros((cols * m, dim * n), jnp.bfloat16)
    for k in range(m):
        tall = lax.dynamic_update_slice(tall, swap(wide, k, "expert") if k else wide, ((mine ^ k) * cols, 0))

    scale_down = jnp.stack([lax.dynamic_slice_in_dim(s, me * own_rows, own_rows) for s in scales])
    return (whole, scale_down, tall.T)


def solution(mesh):
    return jax.shard_map(
        local,
        mesh=mesh,
        in_specs=(
            P("expert", None, "shard"),
            P("expert", None, "shard"),
            P("shard", "expert"),
            P("shard"),
        ),
        out_specs=(P("expert", "shard", None), P("expert", "shard"), P()),
        check_vma=False,
    )
```
